32 devices in a mesh: freq: 8 (over z, y), rows: 4 (over x, core).
Axes of the slice: x: 2, y: 2, z: 4, core: 2. Of those that a mesh axis runs over, the one named last changes fastest.
Arguments:
- wavefield: bfloat16 [10240, 32, 1024], P('freq', 'rows'), may hold values from -6 to 6
- u_factors: bfloat16 [2, 16, 4, 256, 512], P(None, 'freq', 'rows'), may hold values from -0.25 to 0.25
- v_factors: bfloat16 [2, 16, 4, 512, 256], P(None, 'freq', 'rows'), may hold values from -0.375 to 0.375
- tile_ranks: int32 [16, 4, 40], P('freq', 'rows'), may hold values from 1 to 64, as said below
- tile_offsets: int32 [16, 4, 40], P('freq', 'rows'), may hold values from 0 to 511, as said below
Outputs:
- convolved: bfloat16 [1024, 32, 1024], P(('rows', 'freq'))
The draws below stay inside these ranges and needn't reach their ends.
Inputs may be any that keep to these rules, and one draw needn't show every extreme that they name: tile_ranks[k, i, j] is the rank of tile (i, j) of frequency k; the ranks of one tile row sum to at most 512, exactly 512 on some row of every draw, and every tile row has a tile of rank 64. tile_offsets[k, i, j] is the sum of tile_ranks[k, i, j2] over j2 < j.
All inputs are finite; a program needn't handle non-finite values.
Results may differ from the reference program's by a relative error of at most 0.0072.
Values may be sent and summed in bfloat16 or wider, within the bound.
A program may use at most 128 MiB of HBM per device.

```python
import math
import jax
import jax.numpy as jnp
from jax import lax

RECEIVERS = 10240
SAMPLES = 1024
TILE = 256
RANK_MAX = 64
SLOTS = 512
SOURCES = 32
FREQS = 16
TILE_ROWS = 4
TILE_COLS = 40


def rank_tables(key):
    base_key = jax.random.fold_in(key, 4242)
    key_weight, key_target, key_chosen, key_peak = jax.random.split(base_key, 4)
    weight = jax.random.randint(key_weight, (FREQS, TILE_ROWS, TILE_COLS), 1, 65)
    weight = weight * weight // 64 + 1
    target = SLOTS // 2 + jax.random.randint(key_target, (FREQS, TILE_ROWS), 0, SLOTS - SLOTS // 2 + 1)
    chosen = jax.random.randint(key_chosen, (), 0, FREQS * TILE_ROWS)
    row_number = jnp.arange(FREQS * TILE_ROWS, dtype=jnp.int32).reshape(FREQS, TILE_ROWS)
    target = jnp.where(row_number == chosen, SLOTS, target)
    peak_tile = jax.random.randint(key_peak, (FREQS, TILE_ROWS, 1), 0, TILE_COLS)
    is_peak = jnp.arange(TILE_COLS, dtype=jnp.int32)[None, None, :] == peak_tile
    spare_slots = target - (TILE_COLS - 1) - RANK_MAX
    others = jnp.where(is_peak, 0, weight)
    weight_sum = jnp.sum(others, axis=2)
    base_rank = jnp.minimum(1 + others * spare_slots[:, :, None] // weight_sum[:, :, None], RANK_MAX)
    rank_table = jnp.where(is_peak, RANK_MAX, base_rank)
    deficit = target - jnp.sum(rank_table, axis=2)
    headroom = jnp.where(is_peak, 0, RANK_MAX - rank_table)
    before = jnp.cumsum(headroom, axis=2) - headroom
    rank_table = rank_table + jnp.clip(deficit[:, :, None] - before, 0, headroom)
    starts = jnp.cumsum(rank_table, axis=2) - rank_table
    return (rank_table.astype(jnp.int32), starts.astype(jnp.int32))


def draw_tile_ranks(key, part):
    return rank_tables(key)[0]


def draw_tile_offsets(key, part):
    return rank_tables(key)[1]


def level_of(rng, shape, cuts, least, top_value):
    def one(dim, parts):
        steps = jax.random.uniform(jax.random.fold_in(jax.random.fold_in(rng, 6), dim), (parts,), jnp.float32, least / len(cuts), top_value / len(cuts))
        return jnp.repeat(jnp.exp(steps), shape[dim] // parts).reshape((-1,) + (1,) * (len(shape) - dim - 1))

    gain = one(*cuts[0])
    for cut in cuts[1:]:
        gain = gain * one(*cut)
    return gain


def gaussian(stream_key, shape, spread, most, shards=(), kind=jnp.bfloat16):
    entries = jax.random.normal(stream_key, shape, jnp.float32) * spread
    if len(shards) > 0:
        entries = level_of(stream_key, shape, shards, -0.22, 0.18) * entries
    return jnp.clip(entries, min=-most, max=most).astype(kind)


def setup_inputs(seed: int = 0) -> dict:
    seeds = jax.random.split(jax.random.key(seed), 6)
    return {
        "wavefield": gaussian(seeds[0], (RECEIVERS, SOURCES, SAMPLES), 1.0, 6.0, ((0, 8), (1, 4))),
        "u_factors": gaussian(seeds[1], (2, FREQS, TILE_ROWS, TILE, SLOTS), SLOTS ** -0.5, 0.25, ((1, 8), (2, 4))),
        "v_factors": gaussian(seeds[2], (2, FREQS, TILE_ROWS, SLOTS, TILE), TILE ** -0.5, 0.375, ((1, 8), (2, 4))),
        "tile_ranks": draw_tile_ranks(jax.random.fold_in(seeds[5], 71), 0),
        "tile_offsets": draw_tile_offsets(jax.random.fold_in(seeds[5], 71), 0),
    }


def spectral_tables(freq_count, sample_count):
    freq_bins = jnp.arange(freq_count, dtype=jnp.int32) + 1
    sample_index = jnp.arange(sample_count, dtype=jnp.int32)
    phase_int = freq_bins[:, None] * sample_index[None, :] % sample_count
    angles = phase_int.astype(jnp.float32) * (2.0 * math.pi / sample_count)
    cosine = jnp.cos(angles)
    minus_sine = -jnp.sin(angles)
    stacked = jnp.stack([cosine, minus_sine], axis=1)
    forward = (stacked / math.sqrt(sample_count)).astype(jnp.bfloat16)
    inverse = (stacked / math.sqrt(freq_count)).astype(jnp.bfloat16)
    return (forward, inverse)

def tile_windows(v_row, u_row, starts, rank_max):
    columns = starts.shape[0]
    slot_index = (starts[:, None] + jnp.arange(rank_max, dtype=jnp.int32)[None, :]).reshape(-1)
    v_padded = jnp.pad(v_row, ((0, 0), (0, rank_max), (0, 0)))
    u_padded = jnp.pad(u_row, ((0, 0), (0, 0), (0, rank_max)))
    v_win = jnp.take(v_padded, slot_index, axis=1).reshape(2, columns, rank_max, v_row.shape[2])
    u_win = jnp.take(u_padded, slot_index, axis=2).reshape(2, u_row.shape[1], columns, rank_max)
    return (v_win, u_win)

def tile_row_product(u_row, v_row, counts, starts, spectra):
    v_win, u_win = tile_windows(v_row, u_row, starts, RANK_MAX)
    quadrants = jnp.einsum('ajmr,jbrs->abjms', v_win.astype(jnp.float32), spectra.astype(jnp.float32))
    real_part = quadrants[0, 0] - quadrants[1, 1]
    imag_part = quadrants[0, 1] + quadrants[1, 0]
    rank_mask = jnp.arange(RANK_MAX, dtype=jnp.int32)[None, :] < counts[:, None]
    coeffs = jnp.where(rank_mask[None, :, :, None], jnp.stack([real_part, imag_part]), 0.0).astype(jnp.bfloat16)
    products = jnp.einsum('arjm,cjms->acrs', u_win.astype(jnp.float32), coeffs.astype(jnp.float32))
    return jnp.stack([products[0, 0] - products[1, 1], products[0, 1] + products[1, 0]]).astype(jnp.bfloat16)

def reference(wavefield, u_factors, v_factors, tile_ranks, tile_offsets):
    receivers, sources, samples = wavefield.shape
    freqs = u_factors.shape[1]
    tile_rows = u_factors.shape[2]
    tile_size = u_factors.shape[3]
    columns = receivers // tile_size
    forward, inverse = spectral_tables(freqs, samples)
    blocks = wavefield.reshape(columns, tile_size, sources, samples)

    def transform(block):
        return jnp.einsum('kct,rst->kcrs', forward.astype(jnp.float32), block.astype(jnp.float32)).astype(jnp.bfloat16)
    spectrum = jnp.moveaxis(lax.map(transform, blocks), 1, 0)

    def one_band(items):
        spectra, u_band, v_band, counts, starts = items
        rows_out = [tile_row_product(u_band[:, tile_row], v_band[:, tile_row], counts[tile_row], starts[tile_row], spectra) for tile_row in range(tile_rows)]
        return jnp.stack(rows_out, axis=1)
    bands = lax.map(one_band, (spectrum, jnp.moveaxis(u_factors, 1, 0), jnp.moveaxis(v_factors, 1, 0), tile_ranks, tile_offsets))
    flat_bands = bands.reshape(freqs, 2, tile_rows * tile_size * sources)
    series = jnp.einsum('kcq,kct->qt', flat_bands.astype(jnp.float32), inverse.astype(jnp.float32))
    return series.reshape(tile_rows * tile_size, sources, samples).astype(jnp.bfloat16)
```

```python
import functools
import math

import jax
import jax.numpy as jnp
import numpy as np
from jax import lax
from jax.experimental import pallas as pl
from jax.experimental.pallas import tpu as pltpu
from jax.sharding import PartitionSpec as P

RANK_MAX = 64
MESH = pl.DeviceIdType.MESH
LANES = 128


def spectral_tables(freq_count, sample_count):
    freq_bins = jnp.arange(freq_count, dtype=jnp.int32) + 1
    sample_index = jnp.arange(sample_count, dtype=jnp.int32)
    phase_int = freq_bins[:, None] * sample_index[None, :] % sample_count
    angles = phase_int.astype(jnp.float32) * (2.0 * math.pi / sample_count)
    cosine = jnp.cos(angles)
    minus_sine = -jnp.sin(angles)
    stacked = jnp.stack([cosine, minus_sine], axis=1)
    forward = (stacked / math.sqrt(sample_count)).astype(jnp.bfloat16)
    inverse = (stacked / math.sqrt(freq_count)).astype(jnp.bfloat16)
    return (forward, inverse)


def tile_windows(v_row, u_row, starts, rank_max):
    columns = starts.shape[0]
    slot_index = (starts[:, None] + jnp.arange(rank_max, dtype=jnp.int32)[None, :]).reshape(-1)
    v_padded = jnp.pad(v_row, ((0, 0), (0, rank_max), (0, 0)))
    u_padded = jnp.pad(u_row, ((0, 0), (0, 0), (0, rank_max)))
    v_win = jnp.take(v_padded, slot_index, axis=1).reshape(2, columns, rank_max, v_row.shape[2])
    u_win = jnp.take(u_padded, slot_index, axis=2).reshape(2, u_row.shape[1], columns, rank_max)
    return (v_win, u_win)


def slot_lookup(starts, counts, rank_max, slot_count):
    position = jnp.arange(slot_count, dtype=jnp.int32)
    started = starts[:, None, :] <= position[None, :, None]
    owner_tile = jnp.sum(started.astype(jnp.int32), axis=2) - 1
    first_slot = jnp.max(jnp.where(started, starts[:, None, :], 0), axis=2)
    within = position[None, :] - first_slot
    live_slot = position[None, :] < (starts[:, -1] + counts[:, -1])[:, None]
    flat_index = jnp.where(live_slot, owner_tile * rank_max + within, 0)
    return (flat_index, live_slot)


def take_slots(values, chosen):
    return jnp.take(values, chosen, axis=1)


def general_device(wavefield, u_factors, v_factors, tile_ranks, tile_offsets):
    rec_dev, src_dev, samples = wavefield.shape
    freq_dev = u_factors.shape[1]
    rows_dev = u_factors.shape[2]
    tile_size = u_factors.shape[3]
    slot_count = u_factors.shape[4]
    freq_group = lax.axis_size("freq")
    row_group = lax.axis_size("rows")
    freqs = freq_dev * freq_group
    receivers = rec_dev * freq_group
    columns = receivers // tile_size
    sources = src_dev * row_group
    forward, inverse = spectral_tables(freqs, samples)
    spectrum = jnp.einsum("kct,rst->kcrs", forward, wavefield, preferred_element_type=jnp.float32)
    spectrum = spectrum.astype(jnp.bfloat16).reshape(freqs, 2, rec_dev * src_dev)
    windows = jax.vmap(
        functools.partial(tile_windows, rank_max=RANK_MAX), in_axes=(1, 1, 0), out_axes=(1, 1)
    )
    rank_slots = jnp.arange(RANK_MAX, dtype=jnp.int32)
    tile_row = 0
    v_win, u_win = windows(
        v_factors[:, :, tile_row], u_factors[:, :, tile_row], tile_offsets[:, tile_row]
    )
    rank_mask = rank_slots[None, None, :] < tile_ranks[:, tile_row, :, None]
    flat_index, live_slot = slot_lookup(
        tile_offsets[:, tile_row], tile_ranks[:, tile_row], RANK_MAX, slot_count
    )
    prepared = [(v_win, u_win, rank_mask, flat_index, live_slot)]
    by_frequency = lax.all_to_all(spectrum, "freq", split_axis=0, concat_axis=2, tiled=True)
    portion = lax.all_gather(by_frequency[None], "rows", axis=0, tiled=True)
    blocks_in = portion.shape[0]
    spectra = portion.reshape(blocks_in, freq_dev, 2, columns, tile_size, src_dev)
    spectra = jnp.transpose(spectra, (1, 2, 3, 4, 0, 5)).reshape(
        freq_dev, 2, columns, tile_size, blocks_in * src_dev
    )
    tile_row = 0
    v_win, u_win, rank_mask, flat_index, live_slot = prepared[tile_row]
    quadrants = jnp.einsum(
        "afjmr,fbjrs->fabjms", v_win, spectra, preferred_element_type=jnp.float32
    )
    coeffs = jnp.stack(
        [quadrants[:, 0, 0] - quadrants[:, 1, 1], quadrants[:, 0, 1] + quadrants[:, 1, 0]], axis=1
    )
    coeffs = jnp.where(rank_mask[:, None, :, :, None], coeffs, 0.0).astype(jnp.bfloat16)
    stacked = coeffs.reshape(freq_dev, 2, columns * RANK_MAX, blocks_in * src_dev)
    packed = jax.vmap(take_slots)(stacked, flat_index)
    packed = jnp.where(live_slot[:, None, :, None], packed, jnp.zeros((), jnp.bfloat16))
    products = jnp.einsum(
        "afrk,fcks->facrs", u_factors[:, :, tile_row], packed, preferred_element_type=jnp.float32
    )
    results = [
        jnp.stack(
            [products[:, 0, 0] - products[:, 1, 1], products[:, 0, 1] + products[:, 1, 0]], axis=1
        )
    ]
    merged = jnp.stack(results, axis=2)
    bands = merged.astype(jnp.bfloat16).reshape(
        freq_dev, 2, rows_dev * tile_size, blocks_in, src_dev
    )
    bands = bands.reshape(freq_dev, 2, rows_dev * tile_size * sources)
    returned = lax.all_to_all(bands, "freq", split_axis=2, concat_axis=0, tiled=True)
    series = jnp.einsum("kcq,kct->qt", returned, inverse, preferred_element_type=jnp.float32)
    return series.astype(jnp.bfloat16).reshape(rows_dev * tile_size // freq_group, sources, samples)


def host_tables(freq_count, sample_count):
    freq_bins = np.arange(freq_count) + 1
    phase = freq_bins[:, None] * np.arange(sample_count)[None, :] % sample_count
    angles = phase * (2.0 * math.pi / sample_count)
    stacked = np.stack([np.cos(angles), -np.sin(angles)], axis=1)
    stacked = stacked.reshape(2 * freq_count, sample_count)
    forward = (stacked / math.sqrt(sample_count)).astype(np.float32)
    inverse = (stacked / math.sqrt(freq_count)).astype(np.float32)
    return forward, inverse


def band_kernel(
    groups, chunks, tile, src_dev,
    wave, table, u_ref, v_ref, starts, counts, out_ref,
    wbuf, spec, send, xbuf, acc, bsend, brecv,
    wsem, sa, ra, sx, rx, sp, rp, sq, rq, sb, rb,
):
    me = lax.axis_index("freq")
    row = lax.axis_index("rows")
    across = lax.rem(row + 2, 4)
    partner = row + 1 - 2 * lax.rem(row, 2)
    piece = send.shape[1] // groups
    freq_dev = u_ref.shape[1]
    slots = u_ref.shape[3]
    chunk_rows = tile * src_dev

    def load(c):
        return pltpu.make_async_copy(
            wave.at[pl.ds(c * chunk_rows, chunk_rows)], wbuf.at[c], wsem.at[c]
        )

    for c in range(chunks):
        load(c).start()

    barrier = pltpu.get_barrier_semaphore()

    def greet(d, carry):
        peer = lax.rem(me + d, groups)
        pl.semaphore_signal(barrier, inc=1, device_id=(peer, row), device_id_type=MESH)
        return carry

    lax.fori_loop(1, groups, greet, 0)
    pl.semaphore_signal(barrier, inc=1, device_id=(me, across), device_id_type=MESH)
    pl.semaphore_signal(barrier, inc=1, device_id=(me, partner), device_id_type=MESH)
    pl.semaphore_wait(barrier, groups + 1)

    def exchange(c, peer, sender):
        return pltpu.make_async_remote_copy(
            src_ref=send.at[c, pl.ds(peer * piece, piece)],
            dst_ref=xbuf.at[c, sender, row],
            send_sem=sa.at[c, peer],
            recv_sem=ra.at[c, sender],
            device_id=(peer, row),
            device_id_type=MESH,
        )

    def forward(c, g, block, target, s_sem, r_sem):
        return pltpu.make_async_remote_copy(
            src_ref=xbuf.at[c, g, block],
            dst_ref=xbuf.at[c, g, block],
            send_sem=s_sem.at[c, g],
            recv_sem=r_sem.at[c, g],
            device_id=(me, target),
            device_id_type=MESH,
        )

    def to_across(c, g, block):
        return forward(c, g, block, across, sx, rx)

    def to_partner(c, g, block):
        return forward(c, g, block, partner, sp, rp)

    def to_partner_far(c, g, block):
        return forward(c, g, block, partner, sq, rq)

    acc[...] = jnp.zeros_like(acc)
    lane_mod = lax.rem(lax.broadcasted_iota(jnp.int32, (tile, LANES), 1), src_dev)
    sub = 512

    def transform(c):
        load(c).wait()

        def block(b, carry):
            rows = pl.ds(pl.multiple_of(b * sub, sub), sub)
            values = lax.dot_general(
                wbuf[c, rows, :], table[...], (((1,), (1,)), ((), ())),
                preferred_element_type=jnp.float32,
            )
            for h in range(spec.shape[0]):
                spec[h, rows, :] = values[:, h * LANES : (h + 1) * LANES]
            return carry

        lax.fori_loop(0, chunk_rows // sub, block, 0)
        for h in range(spec.shape[0]):
            cols = slice(h * LANES, (h + 1) * LANES)
            picked = spec[h, pl.ds(0, tile, stride=src_dev), :]
            for s in range(1, src_dev):
                picked = jnp.where(
                    lane_mod == s, spec[h, pl.ds(s, tile, stride=src_dev), :], picked
                )
            send[c, cols, :] = picked.T.astype(jnp.bfloat16)
        own = pl.multiple_of(me * piece, piece)
        xbuf[c, me, row] = send[c, pl.ds(own, piece), :]

        def start(d, carry):
            exchange(c, lax.rem(me + d, groups), me).start()
            return carry

        lax.fori_loop(1, groups, start, 0)
        to_across(c, me, row).start()
        to_partner(c, me, row).start()

    def relay(c):
        def step(d, carry):
            g = lax.rem(me + groups - d, groups)
            exchange(c, g, g).wait_recv()
            to_across(c, g, row).start()
            to_partner(c, g, row).start()
            return carry

        lax.fori_loop(1, groups, step, 0)

    def relay_far(c):
        def step(d, carry):
            g = lax.rem(me + groups - d, groups)
            to_across(c, g, across).wait_recv()
            to_partner_far(c, g, across).start()
            return carry

        lax.fori_loop(0, groups, step, 0)

    def project(c):
        def arrive(d, carry):
            g = lax.rem(me + groups - d, groups)
            to_partner(c, g, partner).wait_recv()
            to_partner_far(c, g, lax.rem(partner + 2, 4)).wait_recv()
            return carry

        lax.fori_loop(0, groups, arrive, 0)
        slot = lax.broadcasted_iota(jnp.int32, (1, slots), 1)
        half = 2 * src_dev
        for k in range(freq_dev):
            left = xbuf[c, :, :, k * half : (k + 1) * half, :].reshape(groups * 4 * half, tile)
            for a in range(2):
                products = lax.dot_general(
                    left, v_ref[a, k], (((1,), (1,)), ((), ())),
                    preferred_element_type=jnp.float32,
                ).reshape(groups, 4 * half, slots)
                total = acc[k, a]
                for g in range(groups):
                    first = starts[k, g * chunks + c]
                    last = first + counts[k, g * chunks + c]
                    inside = (slot >= first) & (slot < last)
                    total = jnp.where(inside, products[g], total)
                acc[k, a] = total

    def step(c, carry):
        pl.when(c < chunks)(lambda: transform(c))
        pl.when((c >= 1) & (c < chunks + 1))(lambda: relay(c - 1))
        pl.when((c >= 2) & (c < chunks + 2))(lambda: relay_far(c - 2))
        pl.when(c >= 3)(lambda: project(c - 3))
        return carry

    lax.fori_loop(0, chunks + 3, step, 0)

    rows_out = []
    contract = (((1,), (1,)), ((), ()))
    sources = 4 * src_dev
    q_low = LANES // sources
    q_high = tile // groups // q_low
    for k in range(freq_dev):
        first = acc[k, 0].reshape(4, 2, src_dev, slots)
        second = acc[k, 1].reshape(4, 2, src_dev, slots)
        real = (first[:, 0] - second[:, 1]).reshape(sources, slots)
        imag = (first[:, 1] + second[:, 0]).reshape(sources, slots)
        straight = jnp.concatenate([real, imag], axis=0).astype(jnp.bfloat16)
        turned = jnp.concatenate([-imag, real], axis=0).astype(jnp.bfloat16)
        band = lax.dot_general(u_ref[0, k], straight, contract, preferred_element_type=jnp.float32)
        band = band + lax.dot_general(
            u_ref[1, k], turned, contract, preferred_element_type=jnp.float32
        )
        split = band.reshape(groups, q_low, q_high, 2 * sources)
        for part in range(2):
            lanes = slice(part * sources, (part + 1) * sources)
            rows_out.append(
                jnp.concatenate([split[:, q, :, lanes] for q in range(q_low)], axis=-1)
            )
    bsend[...] = jnp.concatenate(rows_out, axis=1).astype(jnp.bfloat16)

    def give_back(peer, sender):
        return pltpu.make_async_remote_copy(
            src_ref=bsend.at[peer],
            dst_ref=brecv.at[sender],
            send_sem=sb.at[peer],
            recv_sem=rb.at[sender],
            device_id=(peer, row),
            device_id_type=MESH,
        )

    def start_back(d, carry):
        give_back(lax.rem(me + d, groups), me).start()
        return carry

    lax.fori_loop(1, groups, start_back, 0)
    brecv[me] = bsend[me]

    def drain(c, carry):
        def one(d, inner):
            g = lax.rem(me + d, groups)
            pl.when(d > 0)(lambda: exchange(c, g, me).wait_send())
            to_across(c, g, row).wait_send()
            to_partner(c, g, row).wait_send()
            to_partner_far(c, g, across).wait_send()
            return inner

        return lax.fori_loop(0, groups, one, carry)

    lax.fori_loop(0, chunks, drain, 0)

    def finish(d, carry):
        peer = lax.rem(me + d, groups)
        give_back(peer, me).wait_send()
        source = lax.rem(me + groups - d, groups)
        give_back(source, source).wait_recv()
        return carry

    lax.fori_loop(1, groups, finish, 0)
    out_ref[...] = brecv[...].reshape(out_ref.shape)


def series_kernel(q_high, band_ref, table_ref, out_ref, wide):
    step = pl.program_id(0)

    @pl.when(step == 0)
    def _():
        wide[...] = band_ref[...].astype(jnp.float32)

    left = wide[pl.ds(step, band_ref.shape[0] // q_high, stride=q_high), :]
    series = jnp.dot(
        left.T.astype(jnp.bfloat16), table_ref[...], preferred_element_type=jnp.float32
    )
    out_ref[...] = series.astype(jnp.bfloat16).reshape(out_ref.shape)


def fast_device(wavefield, u_factors, v_factors, tile_ranks, tile_offsets):
    rec_dev, src_dev, samples = wavefield.shape
    freq_dev, tile, slots = u_factors.shape[1], u_factors.shape[3], u_factors.shape[4]
    groups = lax.axis_size("freq")
    chunks = rec_dev // tile
    forward, inverse = host_tables(freq_dev * groups, samples)
    table = jnp.asarray(np.repeat(forward, src_dev, axis=0)).astype(jnp.bfloat16)
    inverse = jnp.asarray(inverse).astype(jnp.bfloat16)
    columns = table.shape[0]
    piece = columns // groups
    sources = 4 * src_dev
    q_dev = tile // groups
    q_low = LANES // sources
    q_high = q_dev // q_low
    band_rows = 2 * freq_dev * q_high
    vmem = pl.BlockSpec(memory_space=pltpu.VMEM)
    smem = pl.BlockSpec(memory_space=pltpu.SMEM)
    dma = pltpu.SemaphoreType.DMA
    bands = pl.pallas_call(
        functools.partial(band_kernel, groups, chunks, tile, src_dev),
        out_shape=jax.ShapeDtypeStruct((groups * band_rows, LANES), jnp.bfloat16),
        in_specs=[pl.BlockSpec(memory_space=pl.ANY), vmem, vmem, vmem, smem, smem],
        out_specs=vmem,
        scratch_shapes=[
            pltpu.VMEM((chunks, tile * src_dev, samples), jnp.bfloat16),
            pltpu.VMEM((columns // LANES, tile * src_dev, LANES), jnp.float32),
            pltpu.VMEM((chunks, columns, tile), jnp.bfloat16),
            pltpu.VMEM((chunks, groups, 4, piece, tile), jnp.bfloat16),
            pltpu.VMEM((freq_dev, 2, 8 * src_dev, slots), jnp.float32),
            pltpu.VMEM((groups, band_rows, LANES), jnp.bfloat16),
            pltpu.VMEM((groups, band_rows, LANES), jnp.bfloat16),
            dma((chunks,)),
        ]
        + [dma((chunks, groups)) for _ in range(8)]
        + [dma((groups,)), dma((groups,))],
        compiler_params=pltpu.CompilerParams(
            collective_id=0, has_side_effects=True, vmem_limit_bytes=60 * 1024 * 1024
        ),
        name="bands",
    )(
        wavefield.reshape(rec_dev * src_dev, samples),
        table,
        u_factors[:, :, 0],
        v_factors[:, :, 0],
        tile_offsets[:, 0],
        tile_ranks[:, 0],
    )
    series = pl.pallas_call(
        functools.partial(series_kernel, q_high),
        grid=(q_high,),
        out_shape=jax.ShapeDtypeStruct((q_low, q_high, sources, samples), jnp.bfloat16),
        in_specs=[
            pl.BlockSpec(bands.shape, lambda q: (0, 0)),
            pl.BlockSpec(inverse.shape, lambda q: (0, 0)),
        ],
        out_specs=pl.BlockSpec((q_low, 1, sources, samples), lambda q: (0, q, 0, 0)),
        scratch_shapes=[pltpu.VMEM(bands.shape, jnp.float32)],
        name="series",
    )(bands, inverse)
    return series.reshape(q_dev, sources, samples)


def per_device(wavefield, u_factors, v_factors, tile_ranks, tile_offsets):
    rec_dev, src_dev, samples = wavefield.shape
    tile, slots = u_factors.shape[3], u_factors.shape[4]
    groups = lax.axis_size("freq")
    aligned = tile % LANES == 0 and rec_dev % tile == 0 and slots % LANES == 0
    aligned = aligned and samples % LANES == 0
    counts = u_factors.shape[1] == 2 and u_factors.shape[2] == 1 and src_dev == 8
    counts = counts and lax.axis_size("rows") == 4 and groups > 1 and groups * 32 % LANES == 0
    if aligned and counts and tile == groups * 32:
        return fast_device(wavefield, u_factors, v_factors, tile_ranks, tile_offsets)
    return general_device(wavefield, u_factors, v_factors, tile_ranks, tile_offsets)


def solution(mesh):
    placed = (
        P("freq", "rows", None),
        P(None, "freq", "rows", None, None),
        P(None, "freq", "rows", None, None),
        P("freq", "rows", None),
        P("freq", "rows", None),
    )
    return jax.shard_map(
        per_device,
        mesh=mesh,
        in_specs=placed,
        out_specs=P(("rows", "freq"), None, None),
        check_vma=False,
    )
```

```python
import functools
import math

import jax
import jax.numpy as jnp
import numpy as np
from jax import lax
from jax.experimental import pallas as pl
from jax.experimental.pallas import tpu as pltpu
from jax.sharding import PartitionSpec as P

RANK_MAX = 64
MESH = pl.DeviceIdType.MESH
LANES = 128


def spectral_tables(freq_count, sample_count):
    freq_bins = jnp.arange(freq_count, dtype=jnp.int32) + 1
    sample_index = jnp.arange(sample_count, dtype=jnp.int32)
    phase_int = freq_bins[:, None] * sample_index[None, :] % sample_count
    angles = phase_int.astype(jnp.float32) * (2.0 * math.pi / sample_count)
    cosine = jnp.cos(angles)
    minus_sine = -jnp.sin(angles)
    stacked = jnp.stack([cosine, minus_sine], axis=1)
    forward = (stacked / math.sqrt(sample_count)).astype(jnp.bfloat16)
    inverse = (stacked / math.sqrt(freq_count)).astype(jnp.bfloat16)
    return (forward, inverse)


def tile_windows(v_row, u_row, starts, rank_max):
    columns = starts.shape[0]
    slot_index = (starts[:, None] + jnp.arange(rank_max, dtype=jnp.int32)[None, :]).reshape(-1)
    v_padded = jnp.pad(v_row, ((0, 0), (0, rank_max), (0, 0)))
    u_padded = jnp.pad(u_row, ((0, 0), (0, 0), (0, rank_max)))
    v_win = jnp.take(v_padded, slot_index, axis=1).reshape(2, columns, rank_max, v_row.shape[2])
    u_win = jnp.take(u_padded, slot_index, axis=2).reshape(2, u_row.shape[1], columns, rank_max)
    return (v_win, u_win)


def slot_lookup(starts, counts, rank_max, slot_count):
    position = jnp.arange(slot_count, dtype=jnp.int32)
    started = starts[:, None, :] <= position[None, :, None]
    owner_tile = jnp.sum(started.astype(jnp.int32), axis=2) - 1
    first_slot = jnp.max(jnp.where(started, starts[:, None, :], 0), axis=2)
    within = position[None, :] - first_slot
    live_slot = position[None, :] < (starts[:, -1] + counts[:, -1])[:, None]
    flat_index = jnp.where(live_slot, owner_tile * rank_max + within, 0)
    return (flat_index, live_slot)


def take_slots(values, chosen):
    return jnp.take(values, chosen, axis=1)


def general_device(wavefield, u_factors, v_factors, tile_ranks, tile_offsets):
    rec_dev, src_dev, samples = wavefield.shape
    freq_dev = u_factors.shape[1]
    rows_dev = u_factors.shape[2]
    tile_size = u_factors.shape[3]
    slot_count = u_factors.shape[4]
    freq_group = lax.axis_size("freq")
    row_group = lax.axis_size("rows")
    freqs = freq_dev * freq_group
    receivers = rec_dev * freq_group
    columns = receivers // tile_size
    sources = src_dev * row_group
    forward, inverse = spectral_tables(freqs, samples)
    spectrum = jnp.einsum("kct,rst->kcrs", forward, wavefield, preferred_element_type=jnp.float32)
    spectrum = spectrum.astype(jnp.bfloat16).reshape(freqs, 2, rec_dev * src_dev)
    windows = jax.vmap(
        functools.partial(tile_windows, rank_max=RANK_MAX), in_axes=(1, 1, 0), out_axes=(1, 1)
    )
    rank_slots = jnp.arange(RANK_MAX, dtype=jnp.int32)
    tile_row = 0
    v_win, u_win = windows(
        v_factors[:, :, tile_row], u_factors[:, :, tile_row], tile_offsets[:, tile_row]
    )
    rank_mask = rank_slots[None, None, :] < tile_ranks[:, tile_row, :, None]
    flat_index, live_slot = slot_lookup(
        tile_offsets[:, tile_row], tile_ranks[:, tile_row], RANK_MAX, slot_count
    )
    prepared = [(v_win, u_win, rank_mask, flat_index, live_slot)]
    by_frequency = lax.all_to_all(spectrum, "freq", split_axis=0, concat_axis=2, tiled=True)
    portion = lax.all_gather(by_frequency[None], "rows", axis=0, tiled=True)
    blocks_in = portion.shape[0]
    spectra = portion.reshape(blocks_in, freq_dev, 2, columns, tile_size, src_dev)
    spectra = jnp.transpose(spectra, (1, 2, 3, 4, 0, 5)).reshape(
        freq_dev, 2, columns, tile_size, blocks_in * src_dev
    )
    tile_row = 0
    v_win, u_win, rank_mask, flat_index, live_slot = prepared[tile_row]
    quadrants = jnp.einsum(
        "afjmr,fbjrs->fabjms", v_win, spectra, preferred_element_type=jnp.float32
    )
    coeffs = jnp.stack(
        [quadrants[:, 0, 0] - quadrants[:, 1, 1], quadrants[:, 0, 1] + quadrants[:, 1, 0]], axis=1
    )
    coeffs = jnp.where(rank_mask[:, None, :, :, None], coeffs, 0.0).astype(jnp.bfloat16)
    stacked = coeffs.reshape(freq_dev, 2, columns * RANK_MAX, blocks_in * src_dev)
    packed = jax.vmap(take_slots)(stacked, flat_index)
    packed = jnp.where(live_slot[:, None, :, None], packed, jnp.zeros((), jnp.bfloat16))
    products = jnp.einsum(
        "afrk,fcks->facrs", u_factors[:, :, tile_row], packed, preferred_element_type=jnp.float32
    )
    results = [
        jnp.stack(
            [products[:, 0, 0] - products[:, 1, 1], products[:, 0, 1] + products[:, 1, 0]], axis=1
        )
    ]
    merged = jnp.stack(results, axis=2)
    bands = merged.astype(jnp.bfloat16).reshape(
        freq_dev, 2, rows_dev * tile_size, blocks_in, src_dev
    )
    bands = bands.reshape(freq_dev, 2, rows_dev * tile_size * sources)
    returned = lax.all_to_all(bands, "freq", split_axis=2, concat_axis=0, tiled=True)
    series = jnp.einsum("kcq,kct->qt", returned, inverse, preferred_element_type=jnp.float32)
    return series.astype(jnp.bfloat16).reshape(rows_dev * tile_size // freq_group, sources, samples)


def host_tables(freq_count, sample_count):
    freq_bins = np.arange(freq_count) + 1
    phase = freq_bins[:, None] * np.arange(sample_count)[None, :] % sample_count
    angles = phase * (2.0 * math.pi / sample_count)
    stacked = np.stack([np.cos(angles), -np.sin(angles)], axis=1)
    stacked = stacked.reshape(2 * freq_count, sample_count)
    forward = (stacked / math.sqrt(sample_count)).astype(np.float32)
    inverse = (stacked / math.sqrt(freq_count)).astype(np.float32)
    return forward, inverse


def band_kernel(
    groups, chunks, tile, src_dev,
    wave, table, u_hbm, v_hbm, starts, counts, out_ref,
    u_ref, v_ref, wbuf, spec, send, xbuf, acc, bsend, brecv,
    usem, vsem, wsem, sa, ra, sx, rx, sp, rp, sq, rq, sb, rb,
):
    me = lax.axis_index("freq")
    row = lax.axis_index("rows")
    across = lax.rem(row + 2, 4)
    partner = row + 1 - 2 * lax.rem(row, 2)
    piece = send.shape[1] // groups
    freq_dev = u_ref.shape[1]
    slots = u_ref.shape[3]
    chunk_rows = tile * src_dev

    def load(c):
        return pltpu.make_async_copy(
            wave.at[pl.ds(c * chunk_rows, chunk_rows)], wbuf.at[c], wsem.at[c]
        )

    for c in range(chunks):
        load(c).start()
    load_v = pltpu.make_async_copy(v_hbm, v_ref, vsem)
    load_u = pltpu.make_async_copy(u_hbm, u_ref, usem)
    load_v.start()
    load_u.start()

    barrier = pltpu.get_barrier_semaphore()

    def greet(d, carry):
        peer = lax.rem(me + d, groups)
        pl.semaphore_signal(barrier, inc=1, device_id=(peer, row), device_id_type=MESH)
        return carry

    lax.fori_loop(1, groups, greet, 0)
    pl.semaphore_signal(barrier, inc=1, device_id=(me, across), device_id_type=MESH)
    pl.semaphore_signal(barrier, inc=1, device_id=(me, partner), device_id_type=MESH)
    pl.semaphore_wait(barrier, groups + 1)

    def exchange(c, peer, sender):
        return pltpu.make_async_remote_copy(
            src_ref=send.at[c, pl.ds(peer * piece, piece)],
            dst_ref=xbuf.at[c, sender, row],
            send_sem=sa.at[c, peer],
            recv_sem=ra.at[c, sender],
            device_id=(peer, row),
            device_id_type=MESH,
        )

    def forward(c, g, block, target, s_sem, r_sem):
        return pltpu.make_async_remote_copy(
            src_ref=xbuf.at[c, g, block],
            dst_ref=xbuf.at[c, g, block],
            send_sem=s_sem.at[c, g],
            recv_sem=r_sem.at[c, g],
            device_id=(me, target),
            device_id_type=MESH,
        )

    def to_across(c, g, block):
        return forward(c, g, block, across, sx, rx)

    def to_partner(c, g, block):
        return forward(c, g, block, partner, sp, rp)

    def to_partner_far(c, g, block):
        return forward(c, g, block, partner, sq, rq)

    acc[...] = jnp.zeros_like(acc)
    lane_mod = lax.rem(lax.broadcasted_iota(jnp.int32, (tile, LANES), 1), src_dev)
    sub = 2048

    def transform(c):
        load(c).wait()

        def block(b, carry):
            rows = pl.ds(pl.multiple_of(b * sub, sub), sub)
            values = lax.dot_general(
                wbuf[c, rows, :], table[...], (((1,), (0,)), ((), ())),
                preferred_element_type=jnp.float32,
            )
            for h in range(spec.shape[0]):
                spec[h, rows, :] = values[:, h * LANES : (h + 1) * LANES]
            return carry

        lax.fori_loop(0, chunk_rows // sub, block, 0)
        for h in range(spec.shape[0]):
            cols = slice(h * LANES, (h + 1) * LANES)
            picked = spec[h, pl.ds(0, tile, stride=src_dev), :]
            for s in range(1, src_dev):
                picked = jnp.where(
                    lane_mod == s, spec[h, pl.ds(s, tile, stride=src_dev), :], picked
                )
            send[c, cols, :] = picked.T.astype(jnp.bfloat16)
        own = pl.multiple_of(me * piece, piece)
        xbuf[c, me, row] = send[c, pl.ds(own, piece), :]

        def start(d, carry):
            exchange(c, lax.rem(me + d, groups), me).start()
            return carry

        lax.fori_loop(1, groups, start, 0)
        to_across(c, me, row).start()
        to_partner(c, me, row).start()

    def relay(c):
        def step(d, carry):
            g = lax.rem(me + groups - d, groups)
            exchange(c, g, g).wait_recv()
            to_across(c, g, row).start()
            to_partner(c, g, row).start()
            return carry

        lax.fori_loop(1, groups, step, 0)

    def relay_far(c):
        def step(d, carry):
            g = lax.rem(me + groups - d, groups)
            to_across(c, g, across).wait_recv()
            to_partner_far(c, g, across).start()
            return carry

        lax.fori_loop(0, groups, step, 0)

    def project(c):
        def arrive(d, carry):
            g = lax.rem(me + groups - d, groups)
            to_partner(c, g, partner).wait_recv()
            to_partner_far(c, g, lax.rem(partner + 2, 4)).wait_recv()
            return carry

        lax.fori_loop(0, groups, arrive, 0)
        slot = lax.broadcasted_iota(jnp.int32, (1, slots), 1)
        half = 2 * src_dev
        for k in range(freq_dev):
            left = xbuf[c, :, :, k * half : (k + 1) * half, :].reshape(groups * 4 * half, tile)
            for a in range(2):
                products = lax.dot_general(
                    left, v_ref[a, k], (((1,), (1,)), ((), ())),
                    preferred_element_type=jnp.float32,
                ).reshape(groups, 4 * half, slots)
                total = acc[k, a]
                for g in range(groups):
                    first = starts[k, g * chunks + c]
                    last = first + counts[k, g * chunks + c]
                    inside = (slot >= first) & (slot < last)
                    total = jnp.where(inside, products[g], total)
                acc[k, a] = total

    def step(c, carry):
        pl.when(c < chunks)(lambda: transform(c))
        pl.when((c >= 2) & (c < chunks + 2))(lambda: relay(c - 2))
        pl.when((c >= 3) & (c < chunks + 3))(lambda: relay_far(c - 3))
        pl.when(c == 4)(load_v.wait)
        pl.when(c >= 4)(lambda: project(c - 4))
        return carry

    lax.fori_loop(0, chunks + 4, step, 0)

    load_u.wait()
    rows_out = []
    contract = (((1,), (1,)), ((), ()))
    sources = 4 * src_dev
    q_low = LANES // sources
    q_high = tile // groups // q_low
    for k in range(freq_dev):
        first = acc[k, 0].reshape(4, 2, src_dev, slots)
        second = acc[k, 1].reshape(4, 2, src_dev, slots)
        real = (first[:, 0] - second[:, 1]).reshape(sources, slots)
        imag = (first[:, 1] + second[:, 0]).reshape(sources, slots)
        straight = jnp.concatenate([real, imag], axis=0).astype(jnp.bfloat16)
        turned = jnp.concatenate([-imag, real], axis=0).astype(jnp.bfloat16)
        band = lax.dot_general(u_ref[0, k], straight, contract, preferred_element_type=jnp.float32)
        band = band + lax.dot_general(
            u_ref[1, k], turned, contract, preferred_element_type=jnp.float32
        )
        split = band.reshape(groups, q_low, q_high, 2 * sources)
        for part in range(2):
            lanes = slice(part * sources, (part + 1) * sources)
            rows_out.append(
                jnp.concatenate([split[:, q, :, lanes] for q in range(q_low)], axis=-1)
            )
    bsend[...] = jnp.concatenate(rows_out, axis=1).astype(jnp.bfloat16)

    def give_back(peer, sender):
        return pltpu.make_async_remote_copy(
            src_ref=bsend.at[peer],
            dst_ref=brecv.at[sender],
            send_sem=sb.at[peer],
            recv_sem=rb.at[sender],
            device_id=(peer, row),
            device_id_type=MESH,
        )

    def start_back(d, carry):
        give_back(lax.rem(me + d, groups), me).start()
        return carry

    lax.fori_loop(1, groups, start_back, 0)
    brecv[me] = bsend[me]

    def drain(c, carry):
        def one(d, inner):
            g = lax.rem(me + d, groups)
            pl.when(d > 0)(lambda: exchange(c, g, me).wait_send())
            to_across(c, g, row).wait_send()
            to_partner(c, g, row).wait_send()
            to_partner_far(c, g, across).wait_send()
            return inner

        return lax.fori_loop(0, groups, one, carry)

    lax.fori_loop(0, chunks, drain, 0)

    def finish(d, carry):
        peer = lax.rem(me + d, groups)
        give_back(peer, me).wait_send()
        source = lax.rem(me + groups - d, groups)
        give_back(source, source).wait_recv()
        return carry

    lax.fori_loop(1, groups, finish, 0)
    out_ref[...] = brecv[...].reshape(out_ref.shape)


def series_kernel(q_high, band_ref, table_ref, out_ref, wide):
    step = pl.program_id(0)

    @pl.when(step == 0)
    def _():
        wide[...] = band_ref[...].astype(jnp.float32)

    q_low, q_step, sources, samples = out_ref.shape
    for q in range(q_step):
        rows = pl.ds(step * q_step + q, band_ref.shape[0] // q_high, stride=q_high)
        series = jnp.dot(
            wide[rows, :].T.astype(jnp.bfloat16), table_ref[...],
            preferred_element_type=jnp.float32,
        )
        out_ref[:, q] = series.astype(jnp.bfloat16).reshape(q_low, sources, samples)


def fast_device(wavefield, u_factors, v_factors, tile_ranks, tile_offsets):
    rec_dev, src_dev, samples = wavefield.shape
    freq_dev, tile, slots = u_factors.shape[1], u_factors.shape[3], u_factors.shape[4]
    groups = lax.axis_size("freq")
    chunks = rec_dev // tile
    forward, inverse = host_tables(freq_dev * groups, samples)
    table = jnp.asarray(np.repeat(forward.T, src_dev, axis=1)).astype(jnp.bfloat16)
    inverse = jnp.asarray(inverse).astype(jnp.bfloat16)
    columns = table.shape[1]
    piece = columns // groups
    sources = 4 * src_dev
    q_dev = tile // groups
    q_low = LANES // sources
    q_high = q_dev // q_low
    q_step = q_high // math.gcd(q_high, 2)
    band_rows = 2 * freq_dev * q_high
    vmem = pl.BlockSpec(memory_space=pltpu.VMEM)
    hbm = pl.BlockSpec(memory_space=pl.ANY)
    smem = pl.BlockSpec(memory_space=pltpu.SMEM)
    dma = pltpu.SemaphoreType.DMA
    bands = pl.pallas_call(
        functools.partial(band_kernel, groups, chunks, tile, src_dev),
        out_shape=jax.ShapeDtypeStruct((groups * band_rows, LANES), jnp.bfloat16),
        in_specs=[hbm, vmem, hbm, hbm, smem, smem],
        out_specs=vmem,
        scratch_shapes=[
            pltpu.VMEM((2, freq_dev, tile, slots), jnp.bfloat16),
            pltpu.VMEM((2, freq_dev, slots, tile), jnp.bfloat16),
            pltpu.VMEM((chunks, tile * src_dev, samples), jnp.bfloat16),
            pltpu.VMEM((columns // LANES, tile * src_dev, LANES), jnp.float32),
            pltpu.VMEM((chunks, columns, tile), jnp.bfloat16),
            pltpu.VMEM((chunks, groups, 4, piece, tile), jnp.bfloat16),
            pltpu.VMEM((freq_dev, 2, 8 * src_dev, slots), jnp.float32),
            pltpu.VMEM((groups, band_rows, LANES), jnp.bfloat16),
            pltpu.VMEM((groups, band_rows, LANES), jnp.bfloat16),
            dma,
            dma,
            dma((chunks,)),
        ]
        + [dma((chunks, groups)) for _ in range(8)]
        + [dma((groups,)), dma((groups,))],
        compiler_params=pltpu.CompilerParams(
            collective_id=0, has_side_effects=True, vmem_limit_bytes=60 * 1024 * 1024
        ),
        name="bands",
    )(
        wavefield.reshape(rec_dev * src_dev, samples),
        table,
        u_factors[:, :, 0],
        v_factors[:, :, 0],
        tile_offsets[:, 0],
        tile_ranks[:, 0],
    )
    series = pl.pallas_call(
        functools.partial(series_kernel, q_high),
        grid=(q_high // q_step,),
        out_shape=jax.ShapeDtypeStruct((q_low, q_high, sources, samples), jnp.bfloat16),
        in_specs=[
            pl.BlockSpec(bands.shape, lambda q: (0, 0)),
            pl.BlockSpec(inverse.shape, lambda q: (0, 0)),
        ],
        out_specs=pl.BlockSpec((q_low, q_step, sources, samples), lambda q: (0, q, 0, 0)),
        scratch_shapes=[pltpu.VMEM(bands.shape, jnp.float32)],
        name="series",
    )(bands, inverse)
    return series.reshape(q_dev, sources, samples)


def per_device(wavefield, u_factors, v_factors, tile_ranks, tile_offsets):
    rec_dev, src_dev, samples = wavefield.shape
    tile, slots = u_factors.shape[3], u_factors.shape[4]
    groups = lax.axis_size("freq")
    aligned = tile % LANES == 0 and rec_dev % tile == 0 and slots % LANES == 0
    aligned = aligned and samples % LANES == 0
    counts = u_factors.shape[1] == 2 and u_factors.shape[2] == 1 and src_dev == 8
    counts = counts and lax.axis_size("rows") == 4 and groups > 1 and groups * 32 % LANES == 0
    if aligned and counts and tile == groups * 32:
        return fast_device(wavefield, u_factors, v_factors, tile_ranks, tile_offsets)
    return general_device(wavefield, u_factors, v_factors, tile_ranks, tile_offsets)


def solution(mesh):
    placed = (
        P("freq", "rows", None),
        P(None, "freq", "rows", None, None),
        P(None, "freq", "rows", None, None),
        P("freq", "rows", None),
        P("freq", "rows", None),
    )
    return jax.shard_map(
        per_device,
        mesh=mesh,
        in_specs=placed,
        out_specs=P(("rows", "freq"), None, None),
        check_vma=False,
    )
```
